256 devices in a mesh: groups: 2 (over y), dp: 32 (over z, core), mp: 4 (over x).
Axes of the slice: x: 4, y: 2, z: 16, core: 2. Of those that a mesh axis runs over, the one named last changes fastest.
The devices are a block of a 4x16x16 slice.
Arguments:
- tokens: bfloat16 [8192, 7168], P(('groups', 'dp')), parts along dimension 0, may hold values from -20 to 20, as said below
- w_down: bfloat16 [7168, 1536], P('dp', 'mp'), may hold values from -3 to 3, as said below
- gain: float32 [1536], P('mp'), may hold values from 0.25 to 1.75
- w_up: bfloat16 [1536, 26112], P('dp', 'mp'), may hold values from -0.15625 to 0.15625
- head_counts: int32 [4], replicated, may hold values from 30 to 34, as said below
- cotangent: bfloat16 [8192, 26112], P(('groups', 'dp'), 'mp'), parts along dimension 0, may hold values from -6 to 6
Outputs:
- queries: bfloat16 [8192, 26112], P(('groups', 'dp'), 'mp'), parts along dimension 0
- grad_tokens: bfloat16 [8192, 7168], P(('groups', 'dp'), 'mp'), parts along dimension 0
The draws below stay inside these ranges and needn't reach their ends.
There are 2 independent parts, one for each index of `groups`. The reference program is written for one: setup_inputs(seed, part) draws one part's arguments, and reference() takes and returns one part's arrays. A program takes and returns all parts, laid end to end along the dimension named above; an argument that names none is the same for every part. Nothing has to cross between parts.
Inputs may be any that keep to these rules, and one draw needn't show every extreme that they name: `tokens`: hidden states of order one with token scales that differ. `w_down`: entries of order 7168^(-1/2). `head_counts`: the entries sum to 128; one of them is 34.
All inputs are finite; a program needn't handle non-finite values.
Results may differ from the reference program's by a relative error of at most 0.018.
Values may be sent and summed in bfloat16 or wider, within the bound.
No kernel may reach another device: no remote copies, remote signals or barrier semaphores. Data moves between devices by JAX's collectives and lax.ppermute only.
A program may use at most 128 MiB of HBM per device.

```python
import math
import jax
import jax.numpy as jnp
from jax import lax

D = 7168
LAT = 1536
HEADS = 128
HD = 192
HSLOT = 34
TOKENS = 4096
COLS = 26112
N_MP = 4


def draw_tokens(key, part):
    base_key, scale_key = jax.random.split(key, 2)
    values = jnp.clip(jax.random.normal(base_key, (TOKENS, D), jnp.float32), -6.0, 6.0)
    scales = jnp.exp(jax.random.uniform(scale_key, (TOKENS, 1), jnp.float32, math.log(0.3), math.log(3.0)))
    return (values * scales).astype(jnp.bfloat16)


def draw_w_down(key, part):
    base_key, scale_key = jax.random.split(key, 2)
    values = jax.random.normal(base_key, (D, LAT), jnp.float32)
    values = jnp.clip(values, -6.0, 6.0)
    rising = 0.55 + 1.1 * jnp.arange(LAT, dtype=jnp.float32) / LAT
    col_scale = jnp.exp(jax.random.uniform(scale_key, (1, LAT), jnp.float32, -0.7, 0.7)) * rising
    return (values * col_scale * D ** (-0.5)).astype(jnp.bfloat16)


def draw_head_counts(key, part):
    order_key, extra_key = jax.random.split(jax.random.fold_in(key, 11))
    rank_of = jax.random.permutation(order_key, N_MP).astype(jnp.int32)
    excess = HSLOT - HEADS // N_MP
    extra = jax.random.randint(extra_key, (), 0, excess + 1).astype(jnp.int32)
    delta = jnp.where(rank_of == 0, excess, jnp.where(rank_of == 1, -excess, jnp.where(rank_of == 2, extra, jnp.where(rank_of == 3, -extra, 0))))
    return (HEADS // N_MP + delta).astype(jnp.int32)


def shard_levels(stream_key, extent, shards, smallest, top_value):
    def one(axis_at, blocks):
        steps = jax.random.uniform(jax.random.fold_in(jax.random.fold_in(stream_key, 6), axis_at), (blocks,), jnp.float32, smallest / len(shards), top_value / len(shards))
        return jnp.repeat(jnp.exp(steps), extent[axis_at] // blocks).reshape((-1,) + (1,) * (len(extent) - axis_at - 1))

    level = one(*shards[0])
    for cut in shards[1:]:
        level = level * one(*cut)
    return level


def gaussian(own_key, dims, deviation, most, cuts=(), held_as=jnp.bfloat16):
    array = jax.random.normal(own_key, dims, jnp.float32) * deviation
    if len(cuts) > 0:
        array = shard_levels(own_key, dims, cuts, -0.22, 0.18) * array
    return jnp.clip(array, min=-most, max=most).astype(held_as)


def setup_inputs(seed: int = 0, part: int = 0) -> dict:
    keys = jax.random.split(jax.random.key(seed), 7)
    part_keys = jax.random.split(jax.random.fold_in(keys[6], part), 7)
    return {
        "tokens": draw_tokens(jax.random.fold_in(jax.random.fold_in(keys[6], part), 71), part),
        "w_down": draw_w_down(jax.random.fold_in(keys[6], 71), part),
        "gain": jnp.clip(1.0 + 0.15 * jax.random.normal(keys[2], (LAT,), jnp.float32), 0.25, 1.75),
        "w_up": gaussian(keys[3], (LAT, COLS), LAT ** -0.5, 0.15625, ((0, 32), (1, 4))),
        "head_counts": draw_head_counts(jax.random.fold_in(keys[6], 71), part),
        "cotangent": gaussian(part_keys[5], (TOKENS, COLS), 1.0, 6.0, ((0, 32), (1, 4))),
    }


def reference(tokens, w_down, gain, w_up, head_counts, cotangent):
    latent_raw = jnp.dot(tokens, w_down, preferred_element_type=jnp.float32)
    root_mean = jnp.sqrt(lax.optimization_barrier(jnp.mean(latent_raw * latent_raw, axis=1, keepdims=True)) + 1e-06)
    latent = (latent_raw / root_mean * gain).astype(jnp.bfloat16)
    block_cols = HSLOT * HD
    column = jnp.arange(N_MP * block_cols, dtype=jnp.int32)
    owner = column // block_cols
    slot_index = column % block_cols // HD
    keep_mask = (slot_index < head_counts[owner]).astype(jnp.float32)
    queries = (jnp.dot(latent, w_up, preferred_element_type=jnp.float32) * keep_mask).astype(jnp.bfloat16)
    masked = cotangent * keep_mask.astype(jnp.bfloat16)
    grad_latent = lax.dot_general(masked, w_up, (((1,), (1,)), ((), ())), preferred_element_type=jnp.float32)
    inner_dot = lax.optimization_barrier(jnp.sum(gain * grad_latent * latent_raw, axis=1, keepdims=True))
    grad_raw = (gain * grad_latent / root_mean - latent_raw * inner_dot / (LAT * root_mean ** 3)).astype(jnp.bfloat16)
    width = LAT // N_MP
    running = jnp.zeros((tokens.shape[0], D), jnp.float32)
    for block in range(N_MP):
        product = lax.dot_general(grad_raw[:, block * width:(block + 1) * width], w_down[:, block * width:(block + 1) * width], (((1,), (1,)), ((), ())), preferred_element_type=jnp.float32)
        running = running + lax.optimization_barrier(product.astype(jnp.bfloat16)).astype(jnp.float32)
    return (queries, running.astype(jnp.bfloat16))
```

```python
import functools

import jax
import jax.numpy as jnp
from jax import lax
from jax.experimental import pallas as pl
from jax.experimental.pallas import tpu as pltpu
from jax.sharding import Mesh, PartitionSpec as P

HD = 192
LANES = 128
CORES = 2
BF16 = jnp.bfloat16
F32 = jnp.float32


def shifted(array, axis, shift):
    size = lax.axis_size(axis)
    return lax.ppermute(array, axis, [(i, (i + shift) % size) for i in range(size)])


def swapped(array, axis):
    return lax.ppermute(array, axis, [(i, i ^ 1) for i in range(lax.axis_size(axis))])


def ring_blocks(shard, axis):
    size = lax.axis_size(axis)
    half = shard.shape[0] // 2
    found = [(0, 0, shard)]
    up = down = shard
    for step in range(1, size // 2):
        up = shifted(up, axis, 1)
        down = shifted(down, axis, -1)
        found += [(size - step, 0, up), (step, 0, down)]
    found += [
        (size // 2, 0, shifted(up[:half], axis, 1)),
        (size // 2, half, shifted(down[half:], axis, -1)),
    ]
    return found


def place_kernel(places, rows, size, pos_ref, *refs):
    blocks, out_ref = refs[:-1], refs[-1]
    z = pos_ref[0]
    core = pos_ref[1]
    for (offset, first, sibling), block in zip(places, blocks, strict=True):
        owner = lax.rem(z + offset, size)
        member = 1 - core if sibling else core
        start = (owner * CORES + member) * rows + first
        start = pl.multiple_of(start, 16)
        out_ref[pl.ds(start, block.shape[0]), :] = block[...]


def gather_rows(shard):
    size = lax.axis_size("z")
    rows, cols = shard.shape
    places, blocks = [], []
    for offset, first, block in ring_blocks(shard, "z"):
        places += [(offset, first, False), (offset, first, True)]
        blocks += [block, swapped(block, "core")]
    position = jnp.stack([lax.axis_index("z"), lax.axis_index("core")]).astype(jnp.int32)
    total = size * CORES * rows
    return pl.pallas_call(
        functools.partial(place_kernel, places, rows, size),
        out_shape=jax.ShapeDtypeStruct((total, cols), shard.dtype),
        in_specs=[pl.BlockSpec(memory_space=pltpu.SMEM)]
        + [pl.BlockSpec(memory_space=pltpu.VMEM)] * len(blocks),
        out_specs=pl.BlockSpec(memory_space=pltpu.VMEM),
        cost_estimate=pl.CostEstimate(
            flops=total * cols * 64, bytes_accessed=total * cols * 4, transcendentals=0
        ),
        name="place_rows",
    )(position, *blocks)


def contract_last(left, right):
    return lax.dot_general(left, right, (((1,), (1,)), ((), ())), preferred_element_type=F32)


def columns(array, start, width):
    return lax.dynamic_slice_in_dim(array, start, width, 1)


def gathered_columns(array, axis):
    size = lax.axis_size(axis)
    parts = [array] + [shifted(array, axis, -k) for k in range(1, size)]
    twice = jnp.concatenate(parts + parts[:-1], axis=1)
    start = lax.rem(size - lax.axis_index(axis), size) * array.shape[1]
    return columns(twice, start, size * array.shape[1])


def scattered_sum(array, axis, width):
    size = lax.axis_size(axis)
    me = lax.axis_index(axis)
    total = columns(array, me * width, width).astype(F32)
    for k in range(1, size):
        block = columns(array, lax.rem(me + k, size) * width, width)
        total += shifted(block, axis, k).astype(F32)
    return total


def summed(array, axis):
    total = array
    for k in range(1, lax.axis_size(axis)):
        total += shifted(array, axis, k)
    return total


def sent_and_summed(array, axis):
    size = lax.axis_size(axis)
    rows, cols = array.shape
    blocks = jnp.moveaxis(array.reshape(rows, size, cols // size), 1, 0)
    blocks = lax.all_to_all(blocks, axis, 0, 0, tiled=True)
    return jnp.sum(blocks.astype(F32), axis=0)


def body(tokens, w_down, gain, w_up, head_counts, cotangent):
    block_cols = w_up.shape[1]
    rows = tokens.shape[0]
    block_width = w_down.shape[1]
    latent_width = block_width * lax.axis_size("mp")
    tiles = block_cols // LANES
    quarter = -(-tiles // 4) * LANES
    half = 2 * quarter
    late = block_cols - half
    pair = lax.rem(lax.axis_index("groups"), 2)
    core = lax.axis_index("core")

    mine = pair * late
    others = (1 - pair) * late
    held_heads = lax.dynamic_slice_in_dim(head_counts, lax.axis_index("mp"), 1, 0)
    at = jnp.arange(quarter, dtype=jnp.int32) + core * quarter
    kept = ((at + mine) // HD < held_heads).astype(BF16)
    counted = kept * (at + mine >= pair * half).astype(BF16)

    up_half = columns(w_up, mine, half)
    up_own = columns(up_half, core * quarter, quarter)
    up_sib = swapped(columns(up_half, (1 - core) * quarter, quarter), "core")
    up_chip = lax.dynamic_slice_in_dim(
        jnp.concatenate([up_own, up_sib, up_own], axis=0), core * w_up.shape[0], 2 * w_up.shape[0], 0
    )
    up_whole = lax.all_gather(up_chip, "z", axis=0, tiled=True)

    cot_pair = swapped(columns(cotangent, others, half), "groups")
    cot_half = jnp.concatenate([columns(cotangent, mine, half), cot_pair], axis=0)
    cot_sib = swapped(columns(cot_half, (1 - core) * quarter, quarter), "core")
    cot = jnp.concatenate([columns(cot_half, core * quarter, quarter), cot_sib], axis=0) * counted

    down_whole = gather_rows(w_down)
    latent_raw = jnp.dot(tokens, down_whole, preferred_element_type=F32)
    squares = summed(jnp.sum(latent_raw * latent_raw, axis=1), "mp")[:, None]
    root_mean = jnp.sqrt(squares / latent_width + 1e-06)
    latent_local = (latent_raw / root_mean * gain).astype(BF16)
    latent_own = gathered_columns(latent_local, "mp")
    latent_pair = jnp.concatenate([latent_own, swapped(latent_own, "groups")], axis=0)
    latent = jnp.concatenate([latent_pair, swapped(latent_pair, "core")], axis=0)

    up_whole, latent, cot = lax.optimization_barrier((up_whole, latent, cot))
    grad_four = contract_last(cot, up_whole).astype(BF16)
    query_four = (jnp.dot(latent, up_whole, preferred_element_type=F32) * kept.astype(F32)).astype(BF16)

    grad_two = grad_four[: 2 * rows].astype(F32) + swapped(grad_four[2 * rows :], "core").astype(F32)
    grad_two = grad_two.astype(BF16)
    grad_one = grad_two[:rows].astype(F32) + swapped(grad_two[rows:], "groups").astype(F32)
    grad_latent = scattered_sum(grad_one.astype(BF16), "mp", block_width)
    inner_dot = summed(jnp.sum(gain * grad_latent * latent_raw, axis=1), "mp")[:, None]
    grad_raw = (
        gain * grad_latent / root_mean - latent_raw * inner_dot / (latent_width * root_mean**3)
    ).astype(BF16)
    grad_tokens = sent_and_summed(contract_last(grad_raw, down_whole).astype(BF16), "mp").astype(BF16)

    query_own = query_four[: 2 * rows]
    query_sib = swapped(query_four[2 * rows :], "core")
    query_half = columns(jnp.concatenate([query_own, query_sib, query_own], axis=1), core * quarter, half)
    query_pair = swapped(query_half[rows:], "groups")
    query_mine = query_half[:rows]
    early = jnp.where(pair == 0, query_mine, query_pair)
    later = jnp.where(pair == 0, query_pair, query_mine)
    queries = jnp.concatenate([early, later[:, 2 * half - block_cols :]], axis=1)
    return (queries, grad_tokens)


def solution(mesh):
    sizes = mesh.shape
    devices = mesh.devices.reshape(
        sizes["groups"], sizes["dp"] // CORES, CORES, sizes["mp"]
    )
    split = Mesh(devices, ("groups", "z", "core", "mp"))
    in_specs = (
        P(("groups", "z", "core"), None),
        P(("z", "core"), "mp"),
        P("mp"),
        P(("z", "core"), "mp"),
        P(),
        P(("groups", "z", "core"), "mp"),
    )
    out_specs = (P(("groups", "z", "core"), "mp"), P(("groups", "z", "core"), "mp"))
    return jax.shard_map(body, mesh=split, in_specs=in_specs, out_specs=out_specs, check_vma=False)
```

```python
import functools

import jax
import jax.numpy as jnp
from jax import lax
from jax.experimental import pallas as pl
from jax.experimental.pallas import tpu as pltpu
from jax.sharding import Mesh, PartitionSpec as P

HD = 192
LANES = 128
CORES = 2
BF16 = jnp.bfloat16
F32 = jnp.float32


def shifted(array, axis, shift):
    size = lax.axis_size(axis)
    return lax.ppermute(array, axis, [(i, (i + shift) % size) for i in range(size)])


def swapped(array, axis):
    return lax.ppermute(array, axis, [(i, i ^ 1) for i in range(lax.axis_size(axis))])


def ring_shifted(array):
    size = lax.axis_size("z")
    steps = []
    for i in range(size):
        steps.append((i * CORES, (i + 1) % size * CORES))
        steps.append((i * CORES + 1, (i - 1) % size * CORES + 1))
    return lax.ppermute(array, ("z", "core"), steps)


def ring_blocks(shard):
    last = lax.axis_size("z") // 2
    half = shard.shape[0] // 2
    found = [shard]
    for _ in range(1, last):
        found.append(ring_shifted(found[-1]))
    part = lax.dynamic_slice_in_dim(found[-1], lax.axis_index("core") * half, half, 0)
    return found + [ring_shifted(part)]


def chip_rows(own, sibling):
    rows = own.shape[0]
    start = lax.axis_index("core") * rows
    return lax.dynamic_slice_in_dim(jnp.concatenate([own, sibling, own], axis=0), start, 2 * rows, 0)


def place_kernel(moves, rows, size, pos_ref, *refs):
    out_ref = refs[-1]
    z, core = pos_ref[0], pos_ref[1]
    for index, first, height, step, sibling in moves:
        way = 1 - 2 * core if sibling else 2 * core - 1
        start = lax.rem(z + way * step + size, size) * rows
        if height < rows:
            start += height * (1 - core if sibling else core)
        start = pl.multiple_of(start, 16)
        out_ref[pl.ds(start, height)] = refs[index][first : first + height]


def place_rows(size, rows, own, stacks):
    moves = [(step, 0, block.shape[0], step, False) for step, block in enumerate(own)]
    step = 1
    for index, stack in enumerate(stacks):
        first = 0
        while first < stack.shape[0]:
            height = own[step].shape[0]
            moves.append((len(own) + index, first, height, step, True))
            first += height
            step += 1
    operands = [*own, *stacks]
    cols = own[0].shape[1]
    position = jnp.stack([lax.axis_index("z"), lax.axis_index("core")]).astype(jnp.int32)
    return pl.pallas_call(
        functools.partial(place_kernel, moves, rows, size),
        out_shape=jax.ShapeDtypeStruct((size * rows, cols), own[0].dtype),
        in_specs=[pl.BlockSpec(memory_space=pltpu.SMEM)]
        + [pl.BlockSpec(memory_space=pltpu.VMEM)] * len(operands),
        out_specs=pl.BlockSpec(memory_space=pltpu.VMEM),
        cost_estimate=pl.CostEstimate(
            flops=size * rows * cols * 64, bytes_accessed=size * rows * cols * 4, transcendentals=0
        ),
    )(position, *operands)


def contract_last(left, right):
    return lax.dot_general(left, right, (((1,), (1,)), ((), ())), preferred_element_type=F32)


def columns(array, start, width):
    return lax.dynamic_slice_in_dim(array, start, width, 1)


def spread(value):
    high = value.astype(BF16)
    low = (value - high.astype(F32)).astype(BF16)
    lane = lax.broadcasted_iota(jnp.int32, (value.shape[0], LANES), 1)
    zero = jnp.zeros((), BF16)
    return jnp.where(lane == 0, high[:, None], jnp.where(lane == 1, low[:, None], zero))


def gathered(lanes):
    return lanes[:, 0].astype(F32) + lanes[:, 1].astype(F32)


def gathered_columns(array, extra, axis):
    size = lax.axis_size(axis)
    width = array.shape[1]
    parts = [array]
    sent = jnp.concatenate([array, spread(extra)], axis=1)
    for k in range(1, size):
        part = shifted(sent, axis, -k)
        parts.append(part[:, :width])
        extra += gathered(part[:, width:])
    twice = jnp.concatenate(parts + parts[:-1], axis=1)
    start = lax.rem(size - lax.axis_index(axis), size) * width
    return columns(twice, start, size * width), extra


def scattered_sum(array, extra, axis):
    size = lax.axis_size(axis)
    me = lax.axis_index(axis)
    width = array.shape[1] // size
    total = columns(array, me * width, width).astype(F32)
    total_extra = extra
    lanes = spread(extra)
    for k in range(1, size):
        block = columns(array, lax.rem(me + k, size) * width, width).astype(BF16)
        block = shifted(jnp.concatenate([block, lanes], axis=1), axis, k).astype(F32)
        total += block[:, :width]
        total_extra += gathered(block[:, width:])
    return total, total_extra


def projected_sum(left, right, axis):
    size = lax.axis_size(axis)
    assert size == 4
    me = lax.axis_index(axis)
    width = right.shape[0] // size
    half = width // 2

    def product(k):
        rows = lax.dynamic_slice_in_dim(right, lax.rem(me + k, size) * width, width, 0)
        return contract_last(left, rows).astype(BF16)

    far = product(2)
    from_low = shifted(far[:, half:], axis, 1)
    from_high = shifted(far[:, :half], axis, -1)
    up, down, own = product(1), product(3), product(0)
    up = jnp.concatenate(
        [up[:, :half], (up[:, half:].astype(F32) + from_low.astype(F32)).astype(BF16)], axis=1
    )
    down = jnp.concatenate(
        [(down[:, :half].astype(F32) + from_high.astype(F32)).astype(BF16), down[:, half:]], axis=1
    )
    from_low = shifted(up, axis, 1)
    from_high = shifted(down, axis, -1)
    return own.astype(F32) + from_low.astype(F32) + from_high.astype(F32)


def body(tokens, w_down, gain, w_up, head_counts, cotangent):
    block_cols = w_up.shape[1]
    rows = tokens.shape[0]
    block_width = w_down.shape[1]
    latent_width = block_width * lax.axis_size("mp")
    tiles = block_cols // LANES
    quarter = -(-tiles // 4) * LANES
    half = 2 * quarter
    late = block_cols - half
    pair = lax.rem(lax.axis_index("groups"), 2)
    core = lax.axis_index("core")

    mine = pair * late
    others = (1 - pair) * late
    held_heads = lax.dynamic_slice_in_dim(head_counts, lax.axis_index("mp"), 1, 0)
    at = jnp.arange(quarter, dtype=jnp.int32) + core * quarter
    kept = ((at + mine) // HD < held_heads).astype(BF16)
    counted = kept * (at + mine >= pair * half).astype(BF16)

    size = lax.axis_size("z")
    half_ring = size // 2

    down_chip = chip_rows(w_down, swapped(w_down, "core"))
    down_blocks = ring_blocks(down_chip)
    down_sib = swapped(jnp.concatenate(down_blocks[1:], axis=0), "core")
    down_whole = place_rows(size, down_chip.shape[0], down_blocks, [down_sib])

    up_half = columns(w_up, mine, half)
    up_chip = chip_rows(up_half, swapped(up_half, "core"))
    own_blocks = ring_blocks(columns(up_chip, core * quarter, quarter))
    sib_blocks = ring_blocks(columns(up_chip, (1 - core) * quarter, quarter))
    cut = half_ring - 1
    stacks = [
        swapped(jnp.concatenate(sib_blocks[1:cut], axis=0), "core"),
        swapped(jnp.concatenate(sib_blocks[cut:], axis=0), "core"),
    ]
    up_whole = place_rows(size, up_chip.shape[0], own_blocks, stacks)

    cot_pair = swapped(columns(cotangent, others, half), "groups")
    cot_half = jnp.concatenate([columns(cotangent, mine, half), cot_pair], axis=0)
    cot_sib = swapped(columns(cot_half, (1 - core) * quarter, quarter), "core")
    cot = jnp.concatenate([columns(cot_half, core * quarter, quarter), cot_sib], axis=0) * counted

    tokens_pair = jnp.concatenate([tokens, swapped(tokens, "groups")], axis=0)
    raw_pair = jnp.dot(tokens_pair, down_whole, preferred_element_type=F32)
    squares = jnp.sum(raw_pair * raw_pair, axis=1)
    scaled, squares = gathered_columns((raw_pair * gain).astype(BF16), squares, "mp")
    scaled_sib = swapped(jnp.concatenate([scaled, spread(squares)], axis=1), "core")
    squares_four = jnp.concatenate([squares, gathered(scaled_sib[:, latent_width:])])
    scaled_four = jnp.concatenate([scaled, scaled_sib[:, :latent_width]], axis=0)
    root_four = jnp.sqrt(squares_four / latent_width + 1e-06)[:, None]
    root_mean = root_four[:rows]
    latent_raw = raw_pair[:rows]

    grad_four = contract_last(cot, up_whole).astype(BF16)
    query_four = jnp.dot(scaled_four, up_whole, preferred_element_type=F32)
    query_four = (query_four / root_four * kept.astype(F32)).astype(BF16)

    grad_two = grad_four[: 2 * rows].astype(F32) + swapped(grad_four[2 * rows :], "core").astype(F32)
    grad_sent = swapped(grad_two[rows:].astype(BF16), "groups")
    grad_one = grad_two[:rows] + grad_sent.astype(F32)
    inner = jnp.sum(grad_one * scaled[:rows].astype(F32), axis=1)
    grad_latent, inner = scattered_sum(grad_one, inner, "mp")
    inner_dot = inner[:, None]
    grad_raw = (
        gain * grad_latent / root_mean - latent_raw * inner_dot / (latent_width * root_mean**3)
    ).astype(BF16)
    grad_tokens = projected_sum(grad_raw, down_whole, "mp").astype(BF16)

    query_own = query_four[: 2 * rows]
    query_sib = swapped(query_four[2 * rows :], "core")
    query_half = columns(jnp.concatenate([query_own, query_sib, query_own], axis=1), core * quarter, half)
    query_pair = swapped(query_half[rows:], "groups")
    query_mine = query_half[:rows]
    early = jnp.where(pair == 0, query_mine, query_pair)
    later = jnp.where(pair == 0, query_pair, query_mine)
    queries = jnp.concatenate([early, later[:, 2 * half - block_cols :]], axis=1)
    return (queries, grad_tokens)


def solution(mesh):
    sizes = mesh.shape
    size = sizes["dp"] // CORES
    devices = mesh.devices.reshape(sizes["groups"], size, CORES, sizes["mp"])
    split = Mesh(devices, ("groups", "z", "core", "mp"))
    in_specs = (
        P(("groups", "z", "core"), None),
        P(("z", "core"), "mp"),
        P("mp"),
        P(("z", "core"), "mp"),
        P(),
        P(("groups", "z", "core"), "mp"),
    )
    out_specs = (P(("groups", "z", "core"), "mp"), P(("groups", "z", "core"), "mp"))
    return jax.shard_map(body, mesh=split, in_specs=in_specs, out_specs=out_specs, check_vma=False)
```

```python
import functools

import jax
import jax.numpy as jnp
from jax import lax
from jax.experimental import pallas as pl
from jax.experimental.pallas import tpu as pltpu
from jax.sharding import Mesh, PartitionSpec as P

HD = 192
LANES = 128
CORES = 2
BF16 = jnp.bfloat16
F32 = jnp.float32


VMEM = pl.BlockSpec(memory_space=pltpu.VMEM)
SMEM = pl.BlockSpec(memory_space=pltpu.SMEM)


def shifted(array, axis, shift):
    size = lax.axis_size(axis)
    return lax.ppermute(array, axis, [(i, (i + shift) % size) for i in range(size)])


def swapped(array, axis):
    return lax.ppermute(array, axis, [(i, i ^ 1) for i in range(lax.axis_size(axis))])


def ring_shifted(array):
    size = lax.axis_size("z")
    steps = []
    for i in range(size):
        steps.append((i * CORES, (i + 1) % size * CORES))
        steps.append((i * CORES + 1, (i - 1) % size * CORES + 1))
    return lax.ppermute(array, ("z", "core"), steps)


def ring_blocks(shard):
    last = lax.axis_size("z") // 2
    half = shard.shape[0] // 2
    found = [shard]
    for _ in range(1, last):
        found.append(ring_shifted(found[-1]))
    part = lax.dynamic_slice_in_dim(found[-1], lax.axis_index("core") * half, half, 0)
    return found + [ring_shifted(part)]


def chip_rows(own, sibling):
    rows = own.shape[0]
    start = lax.axis_index("core") * rows
    return lax.dynamic_slice_in_dim(jnp.concatenate([own, sibling, own], axis=0), start, 2 * rows, 0)


def local_call(kernel, outs, operands, flops, scratch=()):
    moved = sum(x.size * x.dtype.itemsize for x in [*operands[1:], *outs])
    return pl.pallas_call(
        kernel,
        out_shape=outs,
        in_specs=[SMEM] + [VMEM] * (len(operands) - 1),
        out_specs=[VMEM] * len(outs),
        scratch_shapes=scratch,
        cost_estimate=pl.CostEstimate(flops=flops, bytes_accessed=moved, transcendentals=0),
    )(*operands)


def spread(value):
    high = value.astype(BF16).astype(F32)
    low = value - high
    lane = lax.broadcasted_iota(jnp.int32, (value.shape[0], LANES), 1)
    return jnp.where(lane == 0, high, jnp.where(lane == 1, low, 0.0)).astype(BF16)


def gathered(lanes):
    return jnp.sum(lanes.astype(F32), axis=1, keepdims=True)


def project_kernel(size, count, pos_ref, gain_ref, own_ref, pair_ref, *refs):
    blocks, (down_ref, raw_ref, sent_ref, total_ref) = refs[:-4], refs[-4:]
    z, core = pos_ref[0], pos_ref[1]
    rows = blocks[0].shape[0]
    for index, block in enumerate(blocks):
        sibling = index >= count
        step = index - count + 1 if sibling else index
        way = 1 - 2 * core if sibling else 2 * core - 1
        height = block.shape[0]
        start = lax.rem(z + way * step + size, size) * rows
        if height < rows:
            start += height * (1 - core if sibling else core)
        down_ref[pl.ds(pl.multiple_of(start, 16), height)] = block[...]
    total_ref[...] = jnp.zeros_like(total_ref)
    depth = 4 * LANES

    def chunk(k, carry):
        at = pl.ds(pl.multiple_of(k * depth, depth), depth)
        left = jnp.concatenate([own_ref[:, at], pair_ref[:, at]], axis=0)
        total_ref[...] += jnp.dot(left, down_ref[at, :], preferred_element_type=F32)
        return carry

    lax.fori_loop(0, own_ref.shape[1] // depth, chunk, 0)
    raw = total_ref[...]
    raw_ref[...] = raw[: raw_ref.shape[0]]
    width = raw.shape[1]
    sent_ref[:, :width] = (raw * gain_ref[...]).astype(BF16)
    sent_ref[:, width:] = spread(jnp.sum(raw * raw, axis=1, keepdims=True))


def assemble_kernel(size, latent_width, pos_ref, *refs):
    parts, (scaled_ref, root_ref) = refs[:-2], refs[-2:]
    width = latent_width // size
    squares = None
    for k, part in enumerate(parts):
        block = lax.rem(pos_ref[0] + k, size) * width
        scaled_ref[:, pl.ds(pl.multiple_of(block, LANES), width)] = part[:, :width]
        lanes = gathered(part[:, width:])
        squares = lanes if squares is None else squares + lanes
    root = jnp.sqrt(squares / latent_width + 1e-06)
    root_ref[...] = jnp.broadcast_to(root, root_ref.shape)


def blocks_kernel(size, pos_ref, grad_ref, got_ref, scaled_ref, own_ref, inner_ref, *refs):
    sent, total_ref = refs[:-1], refs[-1]
    rows, width = own_ref.shape
    total = grad_ref[:rows, :].astype(F32) + got_ref[...].astype(F32)
    total_ref[...] = total
    inner = jnp.sum(total * scaled_ref[:rows, :].astype(F32), axis=1, keepdims=True)
    inner_ref[...] = jnp.broadcast_to(inner, inner_ref.shape)
    lanes = spread(inner)
    for k in range(size):
        block = pl.multiple_of(lax.rem(pos_ref[0] + k, size) * width, LANES)
        piece = total_ref[:, pl.ds(block, width)]
        if k == 0:
            own_ref[...] = piece
        else:
            sent[k - 1][:, :width] = piece.astype(BF16)
            sent[k - 1][:, width:] = lanes


def raw_grad_kernel(latent_width, pos_ref, gain_ref, own_ref, inner_ref, raw_ref, root_ref, *refs):
    got, out_ref = refs[:-1], refs[-1]
    rows, width = own_ref.shape
    grad = own_ref[...]
    inner = inner_ref[:, :1]
    for part in got:
        grad += part[:, :width].astype(F32)
        inner += gathered(part[:, width:])
    root = root_ref[:rows, :1]
    removed = raw_ref[...] * (inner / (latent_width * root * root * root))
    out_ref[...] = (gain_ref[...] * grad / root - removed).astype(BF16)


def contract_last(left, right):
    return lax.dot_general(left, right, (((1,), (1,)), ((), ())), preferred_element_type=F32)


def columns(array, start, width):
    return lax.dynamic_slice_in_dim(array, start, width, 1)


def projected_sum(left, right, axis):
    size = lax.axis_size(axis)
    assert size == 4
    me = lax.axis_index(axis)
    width = right.shape[0] // size
    half = width // 2

    def product(k):
        rows = lax.dynamic_slice_in_dim(right, lax.rem(me + k, size) * width, width, 0)
        return contract_last(left, rows).astype(BF16)

    far = product(2)
    from_low = shifted(far[:, half:], axis, 1)
    from_high = shifted(far[:, :half], axis, -1)
    up, down, own = product(1), product(3), product(0)
    up = jnp.concatenate(
        [up[:, :half], (up[:, half:].astype(F32) + from_low.astype(F32)).astype(BF16)], axis=1
    )
    down = jnp.concatenate(
        [(down[:, :half].astype(F32) + from_high.astype(F32)).astype(BF16), down[:, half:]], axis=1
    )
    from_low = shifted(up, axis, 1)
    from_high = shifted(down, axis, -1)
    return own.astype(F32) + from_low.astype(F32) + from_high.astype(F32)


def body(tokens, w_down, gain, w_up, head_counts, cotangent):
    block_cols = w_up.shape[1]
    rows, depth = tokens.shape
    width = w_down.shape[1]
    n_mp = lax.axis_size("mp")
    latent_width = width * n_mp
    tiles = block_cols // LANES
    half = -(-tiles // 2) * LANES
    late = block_cols - half
    pair = lax.rem(lax.axis_index("groups"), 2)
    at_mp = lax.axis_index("mp").astype(jnp.int32)[None]
    gain = gain[None, :]

    mine = pair * late
    others = (1 - pair) * late
    held_heads = lax.dynamic_slice_in_dim(head_counts, lax.axis_index("mp"), 1, 0)
    at = jnp.arange(half, dtype=jnp.int32) + mine
    kept = (at // HD < held_heads).astype(BF16)
    counted = kept * (at >= pair * half).astype(BF16)

    up_whole = lax.all_gather(columns(w_up, mine, half), ("z", "core"), axis=0, tiled=True)

    cot_pair = swapped(columns(cotangent, others, half), "groups")
    cot = jnp.concatenate([columns(cotangent, mine, half), cot_pair], axis=0) * counted

    size = lax.axis_size("z")
    position = jnp.stack([lax.axis_index("z"), lax.axis_index("core")]).astype(jnp.int32)
    blocks = ring_blocks(chip_rows(w_down, swapped(w_down, "core")))
    count = len(blocks)
    blocks += [swapped(block, "core") for step, block in enumerate(blocks) if step]
    tokens_pair = swapped(tokens, "groups")
    down_whole, latent_raw, sent = local_call(
        functools.partial(project_kernel, size, count),
        [
            jax.ShapeDtypeStruct((depth, width), BF16),
            jax.ShapeDtypeStruct((rows, width), F32),
            jax.ShapeDtypeStruct((2 * rows, width + LANES), BF16),
        ],
        [position, gain, tokens, tokens_pair, *blocks],
        4 * rows * depth * width,
        [pltpu.VMEM((2 * rows, width), F32)],
    )

    parts = [sent] + [shifted(sent, "mp", -k) for k in range(1, n_mp)]
    scaled, root = local_call(
        functools.partial(assemble_kernel, n_mp, latent_width),
        [
            jax.ShapeDtypeStruct((2 * rows, latent_width), BF16),
            jax.ShapeDtypeStruct((2 * rows, LANES), F32),
        ],
        [at_mp, *parts],
        16 * rows * latent_width,
    )

    grad_two = contract_last(cot, up_whole).astype(BF16)
    query_two = jnp.dot(scaled, up_whole, preferred_element_type=F32)
    query_two = (query_two / root[:, :1] * kept.astype(F32)).astype(BF16)

    grad_got = swapped(grad_two[rows:], "groups")
    block = jax.ShapeDtypeStruct((rows, width + LANES), BF16)
    own, inner, *sent = local_call(
        functools.partial(blocks_kernel, n_mp),
        [
            jax.ShapeDtypeStruct((rows, width), F32),
            jax.ShapeDtypeStruct((rows, LANES), F32),
            *[block] * (n_mp - 1),
        ],
        [at_mp, grad_two, grad_got, scaled],
        16 * rows * latent_width,
        [pltpu.VMEM((rows, latent_width), F32)],
    )
    got = [shifted(x, "mp", k) for k, x in enumerate(sent, 1)]
    (grad_raw,) = local_call(
        functools.partial(raw_grad_kernel, latent_width),
        [jax.ShapeDtypeStruct((rows, width), BF16)],
        [at_mp, gain, own, inner, latent_raw, root, *got],
        64 * rows * width,
    )
    grad_tokens = projected_sum(grad_raw, down_whole, "mp").astype(BF16)

    query_pair = swapped(query_two[rows:], "groups")
    query_mine = query_two[:rows]
    early = jnp.where(pair == 0, query_mine, query_pair)
    later = jnp.where(pair == 0, query_pair, query_mine)
    queries = jnp.concatenate([early, later[:, 2 * half - block_cols :]], axis=1)
    return (queries, grad_tokens)


def solution(mesh):
    sizes = mesh.shape
    size = sizes["dp"] // CORES
    devices = mesh.devices.reshape(sizes["groups"], size, CORES, sizes["mp"])
    split = Mesh(devices, ("groups", "z", "core", "mp"))
    in_specs = (
        P(("groups", "z", "core"), None),
        P(("z", "core"), "mp"),
        P("mp"),
        P(("z", "core"), "mp"),
        P(),
        P(("groups", "z", "core"), "mp"),
    )
    out_specs = (P(("groups", "z", "core"), "mp"), P(("groups", "z", "core"), "mp"))
    return jax.shard_map(body, mesh=split, in_specs=in_specs, out_specs=out_specs, check_vma=False)
```
